32 devices in a mesh: inter: 16 (over z, y, core), intra: 2 (over x).
Axes of the slice: x: 2, y: 2, z: 4, core: 2. Of those that a mesh axis runs over, the one named last changes fastest.
Arguments:
- partials: bfloat16 [32, 16, 5120], P(('inter', 'intra')), may hold values from -6 to 6
- scales: bfloat16 [32, 16, 20], P(('inter', 'intra')), may hold values from 64 to 1024
- overflow_pos: int32 [32, 1], P(('inter', 'intra')), may hold values from -81920 to 81919, as said below
- weights: float32 [16, 5120], P('inter', 'intra'), may hold values from -6 to 6
- exponent: int32 [], replicated, may hold values from 10 to 16
Outputs:
- grad_out: float32 [16, 5120], P('inter', 'intra')
- block_scale: float32 [16, 20], P('inter', 'intra')
- master_out: float32 [16, 5120], P('inter', 'intra')
- new_exponent: int32 [], replicated
- overflow_count: int32 [], replicated
The draws below stay inside these ranges and needn't reach their ends.
Inputs may be any that keep to these rules, and one draw needn't show every extreme that they name: `overflow_pos`: A negative entry means no overflow on that device; otherwise it is the flat position (row times 5120 plus column) of an overflowed value of that device's partial.
All inputs are finite; a program needn't handle non-finite values.
Results may differ from the reference program's by a relative error of at most 0.0005.
Values may be sent and summed in bfloat16 or wider, within the bound.
A program may use at most 64 MiB of HBM per device.

```python
import math
import jax
import jax.numpy as jnp
from jax import lax

D = 5120
BLOCK = 256
ROWS = 16
N_INTRA = 2
DEVICES = 32


def draw_overflow_pos(key, part):
    key_lead, key_more, key_pos, key_neg, key_pick = jax.random.split(jax.random.fold_in(key, 71), 5)
    group_total = DEVICES // N_INTRA
    negative = jax.random.randint(key_neg, (DEVICES, 1), -(ROWS * D), 0, dtype=jnp.int32)
    picked_device = jax.random.randint(key_pick, (), 0, DEVICES, dtype=jnp.int32)
    lead_member = jax.random.randint(key_lead, (group_total,), 0, N_INTRA, dtype=jnp.int32)
    member = jnp.arange(DEVICES, dtype=jnp.int32) % N_INTRA
    is_lead = member == jnp.repeat(lead_member, N_INTRA)
    extra_flag = jax.random.randint(key_more, (DEVICES,), 0, 2, dtype=jnp.int32) == 1
    flagged = jnp.logical_or(is_lead, extra_flag)
    positive = jax.random.randint(key_pos, (DEVICES, 1), 0, ROWS * D, dtype=jnp.int32)
    values = jnp.where(flagged[:, None], positive, negative)
    values = values.at[picked_device, 0].set(jnp.where(is_lead[picked_device], values[picked_device, 0], -(ROWS * D)))
    top_group = picked_device // N_INTRA
    top_device = top_group * N_INTRA + lead_member[top_group]
    return values.at[top_device, 0].set(ROWS * D - 1)


def spiked(array, key, source, target, blocks, factor):
    def block_of(axis_at):
        return (jnp.arange(array.shape[axis_at]) // (array.shape[axis_at] // blocks)).reshape((-1,) + (1,) * (array.ndim - 1 - axis_at))

    first = jax.random.permutation(key, blocks)[block_of(target)]
    far = (block_of(target) + blocks // 2) % blocks
    return jnp.where((block_of(source) == first) | (block_of(source) == far), factor * array, array)


def level_of(rng, extent, shards, low, top_value):
    gain, own = 1.0, jax.random.fold_in(rng, 6)
    for axis_at, parts in shards:
        heights = jnp.exp(jax.random.uniform(jax.random.fold_in(own, axis_at), (parts,), jnp.float32, low / len(shards), top_value / len(shards)))
        gain = gain * jnp.repeat(heights, extent[axis_at] // parts).reshape([-1 if axis == axis_at else 1 for axis in range(len(extent))])
    return gain


def gaussian(stream_key, shape, spread, reach, cuts=(), kind=jnp.bfloat16):
    factor_of = level_of(stream_key, shape, cuts, -0.22, 0.18) if cuts else 1.0
    values = jax.random.normal(stream_key, shape, jnp.float32) * spread * factor_of
    return jnp.minimum(jnp.maximum(values, -reach), reach).astype(kind)


def bell_draw_with(own_key, shape, deviation, reach, cuts, heavy, held_as=jnp.bfloat16):
    entries = deviation * jax.random.normal(own_key, shape, jnp.float32)
    if cuts:
        entries = entries * level_of(own_key, shape, cuts, -0.22, 0.18)
    return jnp.clip(spiked(entries, jax.random.fold_in(own_key, 3), *heavy), -reach, reach).astype(held_as)


def setup_inputs(seed: int = 0) -> dict:
    key_of = jax.random.split(jax.random.key(seed), 6)
    partials = bell_draw_with(key_of[0], (DEVICES, ROWS, D), 1.0, 6.0, ((0, 32),), (0, 1, 16, 2.0))
    scales = jnp.clip(jnp.exp(math.log(1024.0) - 2.7725887 * jax.random.uniform(key_of[1], (DEVICES, ROWS, D // BLOCK), jnp.float32) ** level_of(key_of[1], (DEVICES, ROWS, D // BLOCK), ((0, 32),), -0.2, 0.2)), 64.0, 1024.0).astype(jnp.bfloat16)
    overflow_pos = draw_overflow_pos(jax.random.fold_in(key_of[5], 71), 0)
    weights = gaussian(key_of[3], (ROWS, D), 1.0, 6.0, ((0, 16), (1, 2)), jnp.float32)
    exponent = jax.random.randint(key_of[4], (), 10, 17).astype(jnp.int32)
    return dict(partials=partials, scales=scales, overflow_pos=overflow_pos, weights=weights, exponent=exponent)


def reference(partials, scales, overflow_pos, weights, exponent):
    def add_term(grad_acc, inputs):
        levels, block_scales = inputs
        scaled = levels.astype(jnp.float32).reshape(ROWS, D // BLOCK, BLOCK) * block_scales.astype(jnp.float32)[:, :, None]
        return grad_acc + scaled.reshape(ROWS, D), None

    grad_sum, _ = lax.scan(add_term, jnp.zeros((ROWS, D), jnp.float32), (partials, scales))
    flag_count = jnp.sum((overflow_pos >= 0).astype(jnp.int32))
    grad_out = grad_sum * jnp.exp2(-exponent.astype(jnp.float32))
    block_scale = jnp.max(jnp.abs(grad_out.reshape(ROWS, D // BLOCK, BLOCK)), axis=2) / 127.0
    master_out = jnp.where(flag_count == 0, weights - 0.5 * grad_out, weights)
    new_exponent = exponent - (flag_count > 0).astype(jnp.int32)
    return grad_out, block_scale, master_out, new_exponent, flag_count
```

```python
import functools

import jax
import jax.numpy as jnp
from jax import lax
from jax.experimental import pallas as pl
from jax.experimental.pallas import tpu as pltpu
from jax.sharding import PartitionSpec as P

LANES = 128
ROW_GROUP = 16
SOURCE_GROUP = 32


def exchange(inter_size, intra_size, block_len, x_hbm, s_hbm, pos_ref, out_ref, xv, sv, staged, outgoing, incoming,
             load_sems, own_sem, send_sem, recv_sem):
    total = inter_size * intra_size
    row_total, full_width = xv.shape
    block_total = sv.shape[1]
    share_cols = full_width // intra_size
    half = share_cols // 2
    tiles = half // LANES
    my_inter = lax.axis_index("inter")
    my_intra = lax.axis_index("intra")
    me = my_inter * intra_size + my_intra

    load_x = pltpu.make_async_copy(x_hbm.at[0], xv, load_sems.at[0])
    load_s = pltpu.make_async_copy(s_hbm.at[0], sv, load_sems.at[1])
    load_x.start()
    load_s.start()

    barrier = pltpu.get_barrier_semaphore()

    def peer(k):
        target = lax.rem(me + k, total)
        return target // intra_size, lax.rem(target, intra_size)

    def greet(k, carry):
        pl.semaphore_signal(barrier, inc=1, device_id=peer(k), device_id_type=pl.DeviceIdType.MESH)
        return carry

    lax.fori_loop(1, total, greet, 0)

    load_x.wait()
    load_s.wait()
    flag = jnp.where(pos_ref[0, 0] >= 0, jnp.float32(1), jnp.float32(0))
    lane = lax.broadcasted_iota(jnp.int32, (ROW_GROUP, LANES), 1)
    pick_block = lax.broadcasted_iota(jnp.int32, (block_total, LANES), 0)
    pick_lane = lax.broadcasted_iota(jnp.int32, (block_total, LANES), 1)

    def stage(group, carry):
        first = pl.multiple_of(group * ROW_GROUP, ROW_GROUP)
        rows = pl.ds(first, ROW_GROUP)
        scale_rows = sv[rows, :]
        for b in range(intra_size):
            for h in range(2):
                start = (b * 2 + h) * half
                staged[:, b, h, pl.ds(0, half)] = xv[rows, pl.ds(start, half)].astype(jnp.float32)
                hit = (pick_block == (start + pick_lane * LANES) // block_len) & (pick_lane < tiles)
                spread = jnp.dot(scale_rows, hit.astype(jnp.float32).astype(jnp.bfloat16),
                                 preferred_element_type=jnp.float32)
                staged[:, b, h, pl.ds(half, LANES)] = jnp.where(lane == tiles, flag, spread)
        outgoing[rows] = staged[...].astype(jnp.bfloat16)
        return carry

    lax.fori_loop(0, row_total // ROW_GROUP, stage, 0)

    own = pltpu.make_async_copy(outgoing.at[my_inter, my_intra], incoming.at[me], own_sem)
    own.start()
    pl.semaphore_wait(barrier, total - 1)

    def send(k, carry):
        to_inter, to_intra = peer(k)
        pltpu.make_async_remote_copy(
            src_ref=outgoing.at[to_inter, to_intra],
            dst_ref=incoming.at[me],
            send_sem=send_sem,
            recv_sem=recv_sem,
            device_id=(to_inter, to_intra),
            device_id_type=pl.DeviceIdType.MESH,
        ).start()
        return carry

    lax.fori_loop(1, total, send, 0)
    own.wait()
    others = incoming.at[pl.ds(0, total - 1)]
    pltpu.make_async_copy(others, others, recv_sem).wait()

    def reduce(group, sums):
        sources = pl.ds(group * SOURCE_GROUP, SOURCE_GROUP)
        factors = incoming[sources, :, pl.ds(half, LANES)].astype(jnp.float32)
        added = [
            jnp.sum(incoming[sources, :, pl.ds(t * LANES, LANES)].astype(jnp.float32) * factors[:, :, t:t + 1], axis=0)
            for t in range(tiles)
        ]
        added.append(jnp.sum(factors, axis=0))
        return tuple(s + a for s, a in zip(sums, added))

    sums = tuple(jnp.zeros((2, LANES), jnp.float32) for _ in range(tiles + 1))
    sums = lax.fori_loop(0, total // SOURCE_GROUP, reduce, sums)
    for t in range(tiles):
        for h in range(2):
            out_ref[0:1, pl.ds(h * half + t * LANES, LANES)] = sums[t][h:h + 1]
    out_ref[0:1, pl.ds(share_cols, LANES)] = sums[tiles][0:1]
    pltpu.make_async_copy(others, others, send_sem).wait()


def finish(block_len, sum_ref, w_ref, e_ref, grad_ref, scale_ref, master_ref, exp_ref, count_ref):
    share_cols = w_ref.shape[1]
    blocks = share_cols // block_len
    tiles = share_cols // 2 // LANES
    counts = sum_ref[0:1, pl.ds(share_cols, LANES)]
    lane = lax.broadcasted_iota(jnp.int32, (1, LANES), 1)
    count = jnp.sum(jnp.where(lane == tiles, counts, 0.0)).astype(jnp.int32)
    exponent = e_ref[0, 0]
    unscale = jnp.exp2(jnp.full((1, LANES), -exponent.astype(jnp.float32), jnp.float32))[:, 0:1]
    grad = sum_ref[0:1, pl.ds(0, share_cols)] * unscale
    grad_ref[...] = grad
    weights = w_ref[...]
    master_ref[...] = jnp.where(count == 0, weights - 0.5 * grad, weights)
    block_lane = lax.broadcasted_iota(jnp.int32, (1, blocks), 1)
    largest = jnp.zeros((1, blocks), jnp.float32)
    for n in range(blocks):
        top = jnp.max(jnp.abs(grad[:, n * block_len:(n + 1) * block_len]), axis=1, keepdims=True)
        largest = jnp.where(block_lane == n, top, largest)
    scale_ref[...] = largest / 127.0
    exp_ref[0] = exponent - jnp.where(count > 0, 1, 0)
    count_ref[0] = count


def on_device(partials, scales, overflow_pos, weights, exponent):
    inter_size = lax.axis_size("inter")
    intra_size = lax.axis_size("intra")
    total = inter_size * intra_size
    row_total, full_width = partials.shape[1], partials.shape[2]
    block_total = scales.shape[2]
    block_len = full_width // block_total
    share_cols = full_width // intra_size
    width = share_cols // 2 + LANES
    any_space = pl.BlockSpec(memory_space=pl.ANY)
    vmem = pl.BlockSpec(memory_space=pltpu.VMEM)
    smem = pl.BlockSpec(memory_space=pltpu.SMEM)
    sums = pl.pallas_call(
        functools.partial(exchange, inter_size, intra_size, block_len),
        out_shape=jax.ShapeDtypeStruct((1, share_cols + LANES), jnp.float32),
        in_specs=[any_space, any_space, smem],
        out_specs=vmem,
        scratch_shapes=[
            pltpu.VMEM((row_total, full_width), jnp.bfloat16),
            pltpu.VMEM((row_total, block_total), jnp.bfloat16),
            pltpu.VMEM((ROW_GROUP, intra_size, 2, width), jnp.float32),
            pltpu.VMEM((row_total, intra_size, 2, width), jnp.bfloat16),
            pltpu.VMEM((total, 2, width), jnp.bfloat16),
            pltpu.SemaphoreType.DMA((2,)),
            pltpu.SemaphoreType.DMA,
            pltpu.SemaphoreType.DMA,
            pltpu.SemaphoreType.DMA,
        ],
        compiler_params=pltpu.CompilerParams(collective_id=0, has_side_effects=True),
        name="exchange",
    )(partials, scales, overflow_pos)
    grad_out, block_scale, master_out, new_exponent, count = pl.pallas_call(
        functools.partial(finish, block_len),
        out_shape=(
            jax.ShapeDtypeStruct((1, share_cols), jnp.float32),
            jax.ShapeDtypeStruct((1, share_cols // block_len), jnp.float32),
            jax.ShapeDtypeStruct((1, share_cols), jnp.float32),
            jax.ShapeDtypeStruct((1,), jnp.int32),
            jax.ShapeDtypeStruct((1,), jnp.int32),
        ),
        in_specs=[vmem, vmem, smem],
        out_specs=(vmem, vmem, vmem, smem, smem),
        name="finish",
    )(sums, weights, exponent.reshape(1, 1))
    return grad_out, block_scale, master_out, new_exponent.reshape(()), count.reshape(())


def solution(mesh):
    placed = (
        P(("inter", "intra"), None, None),
        P(("inter", "intra"), None, None),
        P(("inter", "intra"), None),
        P("inter", "intra"),
        P(),
    )
    return jax.shard_map(
        on_device,
        mesh=mesh,
        in_specs=placed,
        out_specs=(P("inter", "intra"), P("inter", "intra"), P("inter", "intra"), P(), P()),
        check_vma=False,
    )
```

```python
import functools

import jax
import jax.numpy as jnp
from jax import lax
from jax.experimental import pallas as pl
from jax.experimental.pallas import tpu as pltpu
from jax.sharding import PartitionSpec as P

LANES = 128
ROW_GROUP = 16
SOURCE_GROUP = 32


def exchange(inter_size, intra_size, block_len, x_hbm, s_hbm, pos_hbm, w_hbm, e_hbm,
             grad_ref, scale_ref, master_ref, whole_ref,
             xv, sv, pos_ref, w_ref, e_ref, staged, outgoing, incoming,
             load_sems, own_sem, send_sem, recv_sem):
    total = inter_size * intra_size
    row_total, full_width = xv.shape
    block_total = sv.shape[1]
    share_cols = full_width // intra_size
    half = share_cols // 2
    tiles = half // LANES
    my_inter = lax.axis_index("inter")
    my_intra = lax.axis_index("intra")
    me = my_inter * intra_size + my_intra

    loads = [
        pltpu.make_async_copy(src, dst, load_sems.at[n])
        for n, (src, dst) in enumerate(
            ((x_hbm.at[0], xv), (s_hbm.at[0], sv), (pos_hbm, pos_ref), (w_hbm, w_ref), (e_hbm, e_ref))
        )
    ]
    for load in loads:
        load.start()

    barrier = pltpu.get_barrier_semaphore()
    paired = total & (total - 1) == 0 and False
    flips = [bit * (1 - 2 * lax.rem(me // bit, 2)) for bit in (2**n for n in range(total.bit_length() - 1))]

    def peer(k):
        if paired:
            target = me + sum(flip for n, flip in enumerate(flips) if k >> n & 1)
        else:
            target = lax.rem(me + k, total)
        return target // intra_size, lax.rem(target, intra_size)

    def each_peer(visit):
        if paired:
            for k in reversed(range(1, total)):
                visit(k)
        else:
            lax.fori_loop(1, total, lambda k, carry: (visit(k), carry)[1], 0)

    def greet(k):
        pl.semaphore_signal(barrier, inc=1, device_id=peer(k), device_id_type=pl.DeviceIdType.MESH)

    if True:
        each_peer(greet)

    for load in loads[:3]:
        load.wait()
    flag = jnp.where(pos_ref[0, 0] >= 0, jnp.float32(1), jnp.float32(0))
    lane = lax.broadcasted_iota(jnp.int32, (ROW_GROUP, LANES), 1)
    pick_block = lax.broadcasted_iota(jnp.int32, (block_total, LANES), 0)
    pick_lane = lax.broadcasted_iota(jnp.int32, (block_total, LANES), 1)

    def stage(group, carry):
        first = pl.multiple_of(group * ROW_GROUP, ROW_GROUP)
        rows = pl.ds(first, ROW_GROUP)
        scale_rows = sv[rows, :]
        for b in range(intra_size):
            for h in range(2):
                start = (b * 2 + h) * half
                staged[:, b, h, pl.ds(0, half)] = xv[rows, pl.ds(start, half)].astype(jnp.float32)
                hit = (pick_block == (start + pick_lane * LANES) // block_len) & (pick_lane < tiles)
                spread = jnp.dot(scale_rows, hit.astype(jnp.float32).astype(jnp.bfloat16),
                                 preferred_element_type=jnp.float32)
                staged[:, b, h, pl.ds(half, LANES)] = jnp.where(lane == tiles, flag, spread)
        outgoing[rows] = staged[...].astype(jnp.bfloat16)
        return carry

    if True:
        lax.fori_loop(0, row_total // ROW_GROUP, stage, 0)

    own = pltpu.make_async_copy(outgoing.at[my_inter, my_intra], incoming.at[me], own_sem)
    own.start()
    if True:
        pl.semaphore_wait(barrier, total - 1)

    def send(k):
        to_inter, to_intra = peer(k)
        pltpu.make_async_remote_copy(
            src_ref=outgoing.at[to_inter, to_intra],
            dst_ref=incoming.at[me],
            send_sem=send_sem,
            recv_sem=recv_sem,
            device_id=(to_inter, to_intra),
            device_id_type=pl.DeviceIdType.MESH,
        ).start()

    if True:
        each_peer(send)
    for load in loads[3:]:
        load.wait()
    exponent = e_ref[0]
    unscale = jnp.exp2(jnp.full((1, LANES), -exponent.astype(jnp.float32), jnp.float32))
    own.wait()
    others = incoming.at[pl.ds(0, total - 1)]
    if True:
        pltpu.make_async_copy(others, others, recv_sem).wait()

    def reduce(group, sums):
        sources = pl.ds(group * SOURCE_GROUP, SOURCE_GROUP)
        factors = incoming[sources, :, pl.ds(half, LANES)].astype(jnp.float32)
        added = [
            jnp.sum(incoming[sources, :, pl.ds(t * LANES, LANES)].astype(jnp.float32) * factors[:, :, t:t + 1], axis=0)
            for t in range(tiles)
        ]
        added.append(jnp.sum(factors, axis=0))
        return tuple(s + a for s, a in zip(sums, added))

    sums = tuple(jnp.zeros((2, LANES), jnp.float32) for _ in range(tiles + 1))
    if True:
        if total == SOURCE_GROUP:
            sums = reduce(0, sums)
        else:
            sums = lax.fori_loop(0, total // SOURCE_GROUP, reduce, sums)
    lane = lax.broadcasted_iota(jnp.int32, (1, LANES), 1)
    count = jnp.sum(jnp.where(lane == tiles, sums[tiles][0:1], 0.0)).astype(jnp.int32)
    blocks = share_cols // block_len
    per_block = block_len // LANES
    block_lane = lax.broadcasted_iota(jnp.int32, (1, blocks), 1)
    largest = jnp.zeros((1, blocks), jnp.float32)
    tops = []
    for h in range(2):
        for t in range(tiles):
            grad = sums[t][h:h + 1] * unscale
            columns = pl.ds(h * half + t * LANES, LANES)
            grad_ref[0:1, columns] = grad
            weights = w_ref[0:1, columns]
            master_ref[0:1, columns] = jnp.where(count == 0, weights - 0.5 * grad, weights)
            tops.append(jnp.abs(grad))
    for n in range(blocks):
        top = functools.reduce(jnp.maximum, tops[n * per_block:(n + 1) * per_block])
        largest = jnp.where(block_lane == n, jnp.max(top, axis=1, keepdims=True), largest)
    scale_ref[...] = largest / 127.0
    whole_ref[0:1, pl.ds(0, LANES)] = jnp.full((1, LANES), exponent - jnp.where(count > 0, 1, 0), jnp.int32)
    whole_ref[0:1, pl.ds(LANES, LANES)] = jnp.full((1, LANES), count, jnp.int32)
    if True:
        pltpu.make_async_copy(others, others, send_sem).wait()


def finish(grad_in, scale_in, master_in, whole_in, grad_ref, scale_ref, master_ref, exp_ref, count_ref, sems):
    copies = [
        pltpu.make_async_copy(src, dst, sems.at[n])
        for n, (src, dst) in enumerate(((grad_in, grad_ref), (scale_in, scale_ref), (master_in, master_ref)))
    ]
    for copy in copies:
        copy.start()
    exp_ref[0] = whole_in[0:1, 0:1][0, 0]
    count_ref[0] = whole_in[0:1, LANES:LANES + 1][0, 0]
    for copy in copies:
        copy.wait()


def on_device(partials, scales, overflow_pos, weights, exponent):
    inter_size = lax.axis_size("inter")
    intra_size = lax.axis_size("intra")
    total = inter_size * intra_size
    row_total, full_width = partials.shape[1], partials.shape[2]
    block_total = scales.shape[2]
    block_len = full_width // block_total
    share_cols = full_width // intra_size
    blocks = share_cols // block_len
    width = share_cols // 2 + LANES
    any_space = pl.BlockSpec(memory_space=pl.ANY)
    vmem = pl.BlockSpec(memory_space=pltpu.VMEM)
    smem = pl.BlockSpec(memory_space=pltpu.SMEM)
    results = pl.pallas_call(
        functools.partial(exchange, inter_size, intra_size, block_len),
        out_shape=(
            pltpu.VMEM((1, share_cols), jnp.float32),
            pltpu.VMEM((1, blocks), jnp.float32),
            pltpu.VMEM((1, share_cols), jnp.float32),
            pltpu.VMEM((1, 2 * LANES), jnp.int32),
        ),
        in_specs=[any_space] * 5,
        out_specs=(vmem, vmem, vmem, vmem),
        scratch_shapes=[
            pltpu.VMEM((row_total, full_width), jnp.bfloat16),
            pltpu.VMEM((row_total, block_total), jnp.bfloat16),
            pltpu.SMEM((1, 1), jnp.int32),
            pltpu.VMEM((1, share_cols), jnp.float32),
            pltpu.SMEM((1,), jnp.int32),
            pltpu.VMEM((ROW_GROUP, intra_size, 2, width), jnp.float32),
            pltpu.VMEM((row_total, intra_size, 2, width), jnp.bfloat16),
            pltpu.VMEM((total, 2, width), jnp.bfloat16),
            pltpu.SemaphoreType.DMA((5,)),
            pltpu.SemaphoreType.DMA,
            pltpu.SemaphoreType.DMA,
            pltpu.SemaphoreType.DMA,
        ],
        compiler_params=pltpu.CompilerParams(collective_id=0, has_side_effects=True),
        name="exchange",
    )(partials, scales, overflow_pos, weights, exponent.reshape(1))
    grad_out, block_scale, master_out, new_exponent, count = pl.pallas_call(
        finish,
        out_shape=(
            jax.ShapeDtypeStruct((1, share_cols), jnp.float32),
            jax.ShapeDtypeStruct((1, blocks), jnp.float32),
            jax.ShapeDtypeStruct((1, share_cols), jnp.float32),
            jax.ShapeDtypeStruct((1,), jnp.int32),
            jax.ShapeDtypeStruct((1,), jnp.int32),
        ),
        in_specs=[vmem] * 4,
        out_specs=(any_space, any_space, any_space, smem, smem),
        scratch_shapes=[pltpu.SemaphoreType.DMA((3,))],
        name="finish",
    )(*(pltpu.with_memory_space_constraint(result, pltpu.VMEM) for result in results))
    return grad_out, block_scale, master_out, new_exponent.reshape(()), count.reshape(())


def solution(mesh):
    placed = (
        P(("inter", "intra"), None, None),
        P(("inter", "intra"), None, None),
        P(("inter", "intra"), None),
        P("inter", "intra"),
        P(),
    )
    return jax.shard_map(
        on_device,
        mesh=mesh,
        in_specs=placed,
        out_specs=(P("inter", "intra"), P("inter", "intra"), P("inter", "intra"), P(), P()),
        check_vma=False,
    )
```

```python
import functools

import jax
import jax.numpy as jnp
from jax import lax
from jax.experimental import pallas as pl
from jax.experimental.pallas import tpu as pltpu
from jax.sharding import PartitionSpec as P

LANES = 128
ROW_GROUP = 16
SOURCE_GROUP = 32


def exchange(inter_size, intra_size, block_len, x_hbm, s_hbm, pos_hbm, w_hbm, e_hbm,
             grad_ref, scale_ref, master_ref, whole_ref,
             xv, sv, pos_ref, w_ref, e_ref, staged, outgoing, incoming,
             load_sems, own_sem, send_sem, recv_sem):
    total = inter_size * intra_size
    row_total, full_width = xv.shape
    block_total = sv.shape[1]
    share_cols = full_width // intra_size
    half = share_cols // 2
    tiles = half // LANES
    my_inter = lax.axis_index("inter")
    my_intra = lax.axis_index("intra")
    me = my_inter * intra_size + my_intra

    loads = [
        pltpu.make_async_copy(src, dst, load_sems.at[n])
        for n, (src, dst) in enumerate(
            ((x_hbm.at[0], xv), (s_hbm.at[0], sv), (pos_hbm, pos_ref), (w_hbm, w_ref), (e_hbm, e_ref))
        )
    ]
    for load in loads:
        load.start()

    barrier = pltpu.get_barrier_semaphore()
    paired = total & (total - 1) == 0 and False
    flips = [bit * (1 - 2 * lax.rem(me // bit, 2)) for bit in (2**n for n in range(total.bit_length() - 1))]

    def peer(k):
        if paired:
            target = me + sum(flip for n, flip in enumerate(flips) if k >> n & 1)
        else:
            target = lax.rem(me + k, total)
        return target // intra_size, lax.rem(target, intra_size)

    def each_peer(visit):
        if paired:
            for k in reversed(range(1, total)):
                visit(k)
        else:
            lax.fori_loop(1, total, lambda k, carry: (visit(k), carry)[1], 0)

    def greet(target):
        pl.semaphore_signal(barrier, inc=1, device_id=(target // intra_size, target % intra_size), device_id_type=pl.DeviceIdType.MESH)

    if True:
        for n in range(total):
            greet(n)

    for load in loads[:3]:
        load.wait()
    flag = jnp.where(pos_ref[0, 0] >= 0, jnp.float32(1), jnp.float32(0))
    lane = lax.broadcasted_iota(jnp.int32, (ROW_GROUP, LANES), 1)
    pick_block = lax.broadcasted_iota(jnp.int32, (block_total, LANES), 0)
    pick_lane = lax.broadcasted_iota(jnp.int32, (block_total, LANES), 1)

    def stage(group, carry):
        first = pl.multiple_of(group * ROW_GROUP, ROW_GROUP)
        rows = pl.ds(first, ROW_GROUP)
        scale_rows = sv[rows, :]
        for b in range(intra_size):
            for h in range(2):
                start = (b * 2 + h) * half
                staged[:, b, h, pl.ds(0, half)] = xv[rows, pl.ds(start, half)].astype(jnp.float32)
                hit = (pick_block == (start + pick_lane * LANES) // block_len) & (pick_lane < tiles)
                spread = jnp.dot(scale_rows, hit.astype(jnp.float32).astype(jnp.bfloat16),
                                 preferred_element_type=jnp.float32)
                staged[:, b, h, pl.ds(half, LANES)] = jnp.where(lane == tiles, flag, spread)
        outgoing[rows] = staged[...].astype(jnp.bfloat16)
        return carry

    if True:
        lax.fori_loop(0, row_total // ROW_GROUP, stage, 0)

    own = pltpu.make_async_copy(outgoing.at[my_inter, my_intra], incoming.at[me], own_sem)
    own.start()
    if True:
        pl.semaphore_wait(barrier, total)

    def send(target):
        to_inter, to_intra = target // intra_size, target % intra_size
        pltpu.make_async_remote_copy(
            src_ref=outgoing.at[to_inter, to_intra],
            dst_ref=incoming.at[me],
            send_sem=send_sem,
            recv_sem=recv_sem,
            device_id=(to_inter, to_intra),
            device_id_type=pl.DeviceIdType.MESH,
        ).start()

    if True:
        for n in range(total - 1):
            send(n + (n >= me).astype(jnp.int32))
    for load in loads[3:]:
        load.wait()
    exponent = e_ref[0]
    unscale = jnp.exp2(jnp.full((1, LANES), -exponent.astype(jnp.float32), jnp.float32))
    own.wait()
    others = incoming.at[pl.ds(0, total - 1)]
    if True:
        pltpu.make_async_copy(others, others, recv_sem).wait()

    def reduce(group, sums):
        sources = pl.ds(group * SOURCE_GROUP, SOURCE_GROUP)
        factors = incoming[sources, :, pl.ds(half, LANES)].astype(jnp.float32)
        added = [
            jnp.sum(incoming[sources, :, pl.ds(t * LANES, LANES)].astype(jnp.float32) * factors[:, :, t:t + 1], axis=0)
            for t in range(tiles)
        ]
        added.append(jnp.sum(factors, axis=0))
        return tuple(s + a for s, a in zip(sums, added))

    sums = tuple(jnp.zeros((2, LANES), jnp.float32) for _ in range(tiles + 1))
    if True:
        if total == SOURCE_GROUP:
            sums = reduce(0, sums)
        else:
            sums = lax.fori_loop(0, total // SOURCE_GROUP, reduce, sums)
    lane = lax.broadcasted_iota(jnp.int32, (1, LANES), 1)
    count = jnp.sum(jnp.where(lane == tiles, sums[tiles][0:1], 0.0)).astype(jnp.int32)
    blocks = share_cols // block_len
    per_block = block_len // LANES
    block_lane = lax.broadcasted_iota(jnp.int32, (1, blocks), 1)
    largest = jnp.zeros((1, blocks), jnp.float32)
    tops = []
    for h in range(2):
        for t in range(tiles):
            grad = sums[t][h:h + 1] * unscale
            columns = pl.ds(h * half + t * LANES, LANES)
            grad_ref[0:1, columns] = grad
            weights = w_ref[0:1, columns]
            master_ref[0:1, columns] = jnp.where(count == 0, weights - 0.5 * grad, weights)
            tops.append(jnp.abs(grad))
    for n in range(blocks):
        top = functools.reduce(jnp.maximum, tops[n * per_block:(n + 1) * per_block])
        largest = jnp.where(block_lane == n, jnp.max(top, axis=1, keepdims=True), largest)
    scale_ref[...] = largest / 127.0
    whole_ref[0:1, pl.ds(0, LANES)] = jnp.full((1, LANES), exponent - jnp.where(count > 0, 1, 0), jnp.int32)
    whole_ref[0:1, pl.ds(LANES, LANES)] = jnp.full((1, LANES), count, jnp.int32)
    if True:
        pltpu.make_async_copy(others, others, send_sem).wait()


def finish(grad_in, scale_in, master_in, whole_in, grad_ref, scale_ref, master_ref, exp_ref, count_ref, sems):
    copies = [
        pltpu.make_async_copy(src, dst, sems.at[n])
        for n, (src, dst) in enumerate(((grad_in, grad_ref), (scale_in, scale_ref), (master_in, master_ref)))
    ]
    for copy in copies:
        copy.start()
    exp_ref[0] = whole_in[0:1, 0:1][0, 0]
    count_ref[0] = whole_in[0:1, LANES:LANES + 1][0, 0]
    for copy in copies:
        copy.wait()


def on_device(partials, scales, overflow_pos, weights, exponent):
    inter_size = lax.axis_size("inter")
    intra_size = lax.axis_size("intra")
    total = inter_size * intra_size
    row_total, full_width = partials.shape[1], partials.shape[2]
    block_total = scales.shape[2]
    block_len = full_width // block_total
    share_cols = full_width // intra_size
    blocks = share_cols // block_len
    width = share_cols // 2 + LANES
    any_space = pl.BlockSpec(memory_space=pl.ANY)
    vmem = pl.BlockSpec(memory_space=pltpu.VMEM)
    smem = pl.BlockSpec(memory_space=pltpu.SMEM)
    results = pl.pallas_call(
        functools.partial(exchange, inter_size, intra_size, block_len),
        out_shape=(
            pltpu.VMEM((1, share_cols), jnp.float32),
            pltpu.VMEM((1, blocks), jnp.float32),
            pltpu.VMEM((1, share_cols), jnp.float32),
            pltpu.VMEM((1, 2 * LANES), jnp.int32),
        ),
        in_specs=[any_space] * 5,
        out_specs=(vmem, vmem, vmem, vmem),
        scratch_shapes=[
            pltpu.VMEM((row_total, full_width), jnp.bfloat16),
            pltpu.VMEM((row_total, block_total), jnp.bfloat16),
            pltpu.SMEM((1, 1), jnp.int32),
            pltpu.VMEM((1, share_cols), jnp.float32),
            pltpu.SMEM((1,), jnp.int32),
            pltpu.VMEM((ROW_GROUP, intra_size, 2, width), jnp.float32),
            pltpu.VMEM((row_total, intra_size, 2, width), jnp.bfloat16),
            pltpu.VMEM((total, 2, width), jnp.bfloat16),
            pltpu.SemaphoreType.DMA((5,)),
            pltpu.SemaphoreType.DMA,
            pltpu.SemaphoreType.DMA,
            pltpu.SemaphoreType.DMA,
        ],
        compiler_params=pltpu.CompilerParams(collective_id=0, has_side_effects=True),
        name="exchange",
    )(partials, scales, overflow_pos, weights, exponent.reshape(1))
    grad_out, block_scale, master_out, new_exponent, count = pl.pallas_call(
        finish,
        out_shape=(
            jax.ShapeDtypeStruct((1, share_cols), jnp.float32),
            jax.ShapeDtypeStruct((1, blocks), jnp.float32),
            jax.ShapeDtypeStruct((1, share_cols), jnp.float32),
            jax.ShapeDtypeStruct((1,), jnp.int32),
            jax.ShapeDtypeStruct((1,), jnp.int32),
        ),
        in_specs=[vmem] * 4,
        out_specs=(any_space, any_space, any_space, smem, smem),
        scratch_shapes=[pltpu.SemaphoreType.DMA((3,))],
        name="finish",
    )(*(pltpu.with_memory_space_constraint(result, pltpu.VMEM) for result in results))
    return grad_out, block_scale, master_out, new_exponent.reshape(()), count.reshape(())


def solution(mesh):
    placed = (
        P(("inter", "intra"), None, None),
        P(("inter", "intra"), None, None),
        P(("inter", "intra"), None),
        P("inter", "intra"),
        P(),
    )
    return jax.shard_map(
        on_device,
        mesh=mesh,
        in_specs=placed,
        out_specs=(P("inter", "intra"), P("inter", "intra"), P("inter", "intra"), P(), P()),
        check_vma=False,
    )
```
